32 devices in a mesh: lang: 2 (over y), clu: 16 (over z, x, core).
Axes of the slice: x: 2, y: 2, z: 4, core: 2. Of those that a mesh axis runs over, the one named last changes fastest.
Arguments:
- embeddings: bfloat16 [8192, 1024], P(('lang', 'clu')), parts along dimension 0, may hold values from -6 to 6
- assignment: int32 [8192, 1], P(('lang', 'clu')), parts along dimension 0, may hold values from 0 to 31; in each aligned block of 256 rows (0 to 255, 256 to 511, ...) at most 16 rows name the same one
Outputs:
- best_similarity: float32 [8192], P(('lang', 'clu')), parts along dimension 0
The draws below stay inside these ranges and needn't reach their ends.
There are 2 independent parts, one for each index of `lang`. The reference program is written for one: setup_inputs(seed, part) draws one part's arguments, and reference() takes and returns one part's arrays. A program takes and returns all parts, laid end to end along the dimension named above; each array names one. Nothing has to cross between parts.
Inputs may be any that keep to these rules, and one draw needn't show every extreme that they name: `assignment`: in each aligned block of 256 rows (the rows of one device) no cluster is named by more than 16 rows; every cluster is named by some row.
All inputs are finite; a program needn't handle non-finite values.
Results may differ from the reference program's by a relative error of at most 0.0016.
Values may be sent and summed in bfloat16 or wider, within the bound.
A program may use at most 64 MiB of HBM per device.

```python
import math
import jax
import jax.numpy as jnp
import numpy as np
from jax import lax

D = 1024
ROWS_DEV = 256
CLUSTERS = 32
MOST = 16
ROWS = 4096
N_CLU = 16


def shard_levels(rng, extent, shards, least, top_value):
    level = 1.0
    for dim, blocks in shards:
        draws = jax.random.uniform(jax.random.fold_in(jax.random.fold_in(rng, 6), dim), (blocks,), jnp.float32, least / len(shards), top_value / len(shards))
        level = level * jnp.repeat(jnp.exp(draws), extent[dim] // blocks).reshape((-1,) + (1,) * (len(extent) - 1 - dim))
    return level


def deal_out(rng, own, number, rows, amount, top, most, skew):
    ranking = jax.random.permutation(rng, amount)
    crowded, common = portions_of(amount, rows * top, most, skew, True), portions_of(amount, rows * top, most, skew, False)
    places = jnp.arange(amount)

    def named(sizes, turn):
        used = int((sizes > 0).sum())
        fixed = max(1, used // 4)
        moved = fixed + (places - fixed + turn * (used - fixed)) % max(1, amount - fixed)
        return jnp.zeros((amount,), jnp.int32).at[ranking[jnp.where(places < fixed, places, moved)]].set(jnp.asarray(sizes, jnp.int32))

    sizes = jnp.where(number % 4 == 0, named(crowded, number // 4), named(common, number - number // 4 - 1))
    mixed = jax.random.permutation(jax.random.fold_in(own, 3), amount)
    donor, taker = mixed[0:amount // 2 * 2:2], mixed[1:amount // 2 * 2:2]
    margin = jnp.minimum(sizes[donor] - 1, most - sizes[taker]) // 2
    margin = jnp.where((donor == ranking[0]) | (taker == ranking[0]) | (sizes[taker] == 0), 0, jnp.maximum(margin, 0))
    moved = jax.random.randint(jax.random.fold_in(own, 4), (amount // 2,), 0, 1 << 20) % (margin + 1)
    sizes = sizes.at[donor].add(-moved).at[taker].add(moved)
    items = jnp.searchsorted(jnp.cumsum(sizes), jnp.arange(rows * top), side="right").astype(jnp.int32)
    table = items.reshape(top, rows).T
    table = table[jax.random.permutation(jax.random.fold_in(own, 1), rows)]
    turn = jax.random.randint(jax.random.fold_in(own, 2), (rows, 1), 0, top)
    return jnp.take_along_axis(table, (jnp.arange(top)[None, :] + turn) % top, axis=1)


def portions_of(number_of, total, reach, slope, full):
    weights = [(1 << 20) // math.isqrt(standing ** slope) + 1 for standing in range(1, number_of + 1)]
    largest = reach if full else min(reach, max(-(-total // number_of), total * weights[0] // sum(weights)))
    least = 1 if total - largest >= number_of - 1 else 0
    holding, surplus = [largest] + [least] * (number_of - 1), total - largest - least * (number_of - 1)
    while surplus > 0:
        movable = [i for i in range(1, number_of) if holding[i] < largest] or [i for i in range(1, number_of) if holding[i] < reach]
        mass, budget = sum([weights[i] for i in movable]), surplus
        for i in movable:
            extra = min(reach - holding[i], max(1, budget * weights[i] // mass), surplus)
            holding[i] = holding[i] + extra
            surplus = surplus - extra
    return np.array(holding)


def bell_draw(own_key, dims, deviation, most, pieces=(), kind=jnp.bfloat16):
    gain = shard_levels(own_key, dims, pieces, -0.22, 0.18) if pieces else 1.0
    drawn = jax.random.normal(own_key, dims, jnp.float32) * deviation * gain
    return jnp.minimum(jnp.maximum(drawn, -most), most).astype(kind)


def setup_inputs(seed: int = 0, part: int = 0) -> dict:
    splits = jax.random.split(jax.random.key(seed), 3)
    part_splits = jax.random.split(jax.random.fold_in(splits[2], part), 3)
    embeddings = bell_draw(part_splits[0], (ROWS, D), 1.0, 6.0, ((0, 16),))
    assignment_keys = jax.random.split(jax.random.fold_in(part_splits[1], 1), ROWS // ROWS_DEV)
    assignment_turns = jax.random.permutation(jax.random.fold_in(part_splits[1], 3), ROWS // ROWS_DEV)
    assignment = jax.vmap(lambda own, number: deal_out(jax.random.fold_in(part_splits[1], 2), own, number, ROWS_DEV, CLUSTERS, 1, MOST, 2))(assignment_keys, assignment_turns).reshape((ROWS, 1))
    return {"embeddings": embeddings, "assignment": assignment}


EPS = 1e-06

def normalize(embeddings):
    values = embeddings.astype(jnp.float32)
    scale = lax.rsqrt(lax.optimization_barrier(jnp.sum(values * values, axis=-1, keepdims=True)) + EPS)
    return (values * scale).astype(jnp.bfloat16)

def reference(embeddings, assignment):
    unit = normalize(embeddings)
    cluster = assignment[:, 0].astype(jnp.int32)
    total = cluster.shape[0]
    order = jnp.argsort(cluster, stable=True).astype(jnp.int32)
    ranked = cluster[order]
    labels = jnp.arange(CLUSTERS, dtype=jnp.int32)
    starts = jnp.searchsorted(ranked, labels, side='left').astype(jnp.int32)
    ends = jnp.searchsorted(ranked, labels, side='right').astype(jnp.int32)
    sorted_unit = unit[order]
    width = N_CLU * MOST
    offsets = jnp.arange(width, dtype=jnp.int32)
    distinct = offsets[:, None] != offsets[None, :]

    def score(label):
        index = jnp.clip(starts[label] + offsets, 0, total - 1).astype(jnp.int32)
        live = offsets < ends[label] - starts[label]
        rows = sorted_unit[index]
        gram = jnp.dot(rows, rows.T, preferred_element_type=jnp.float32)
        keep = distinct & live[None, :]
        best = lax.optimization_barrier(jnp.max(jnp.where(keep, gram, jnp.float32(-2.0)), axis=1))
        return jnp.maximum(best, jnp.float32(-1.0))
    table = lax.map(score, labels)
    position = jnp.arange(total, dtype=jnp.int32)
    inside = (position - starts[ranked]).astype(jnp.int32)
    sorted_best = table[ranked, inside]
    return jnp.zeros((total,), jnp.float32).at[order].set(sorted_best)
```

```python
import functools

import jax
import jax.numpy as jnp
from jax import lax
from jax.experimental import pallas as pl
from jax.experimental.pallas import tpu as pltpu
from jax.sharding import PartitionSpec as P

CLU_DEV = 2
LANES = 128
EPS = 1e-06
DEAD = 4.0


def normalize(embeddings):
    values = embeddings.astype(jnp.float32)
    scale = lax.rsqrt(jnp.sum(values * values, axis=-1, keepdims=True) + EPS)
    return (values * scale).astype(jnp.bfloat16)


def exchange_kernel(
    groups, most, emb_ref, cluster_ref, out_ref,
    unit, outgoing, arrived, best, returned,
    load_sem, send_sem, recv_sem, back_send_sem, back_recv_sem,
):
    count, width = unit.shape
    block = CLU_DEV * most
    total = groups * block
    me = lax.axis_index("clu")
    chunks = 4
    step = count // chunks

    def load(c):
        rows = pl.ds(c * step, step)
        return pltpu.make_async_copy(emb_ref.at[rows], unit.at[rows], load_sem.at[c])

    for c in range(chunks):
        load(c).start()

    barrier = pltpu.get_barrier_semaphore()
    for k in range(1, groups):
        pl.semaphore_signal(
            barrier, inc=1, device_id={"clu": me ^ k}, device_id_type=pl.DeviceIdType.MESH
        )

    cluster_row = cluster_ref[...]
    row_id = lax.broadcasted_iota(jnp.int32, (count, count), 0)
    col_id = lax.broadcasted_iota(jnp.int32, (count, count), 1)
    spread = jnp.broadcast_to(cluster_row, (count, count))
    cluster_col = jnp.sum(jnp.where(row_id == col_id, spread, 0), axis=1, keepdims=True)
    same = cluster_col == spread
    rank_row = jnp.sum(jnp.where(same & (row_id < col_id), 1, 0), axis=0, keepdims=True)
    slot_row = cluster_row * most + rank_row
    slot_id = lax.broadcasted_iota(jnp.int32, (total, count), 0)
    hit = slot_id == jnp.broadcast_to(slot_row, (total, count))
    place = jnp.where(hit, 1.0, 0.0)
    live = jnp.max(place, axis=1, keepdims=True)
    place = place.astype(jnp.bfloat16)

    for c in range(chunks):
        load(c).wait()
        rows = pl.ds(c * step, step)
        unit[rows, :] = normalize(unit[rows, :])

    outgoing[...] = jnp.dot(
        place, unit[...], preferred_element_type=jnp.float32
    ).astype(jnp.bfloat16)
    lane = lax.broadcasted_iota(jnp.int32, (total, LANES), 1)
    head = outgoing[:, 0:LANES].astype(jnp.float32)
    outgoing[:, 0:LANES] = jnp.where(
        (lane == 0) & (live < 0.5), DEAD, head
    ).astype(jnp.bfloat16)

    pl.semaphore_wait(barrier, groups - 1)

    mine = pl.ds(pl.multiple_of(me * block, block), block)

    def send(k):
        peer = me ^ k
        return pltpu.make_async_remote_copy(
            src_ref=outgoing.at[pl.ds(pl.multiple_of(peer * block, block), block)],
            dst_ref=arrived.at[mine],
            send_sem=send_sem.at[k],
            recv_sem=recv_sem.at[k],
            device_id={"clu": peer},
            device_id_type=pl.DeviceIdType.MESH,
        )

    for k in range(groups - 1, 0, -1):
        send(k).start()
    arrived[mine, :] = outgoing[mine, :]

    rank_col = jnp.sum(
        jnp.where(same & (col_id < row_id), 1, 0), axis=1, keepdims=True
    )
    owner_col = cluster_col // CLU_DEV
    place_col = (cluster_col % CLU_DEV) * most + rank_col + (me * block) % LANES

    for k in range(1, groups):
        send(k).wait()

    rows = arrived[...]
    gram = lax.dot_general(
        rows, rows, (((1,), (1,)), ((), ())), preferred_element_type=jnp.float32
    )
    dead = rows[:, 0:1].astype(jnp.float32) > 2.0
    one = lax.broadcasted_iota(jnp.int32, (total, total), 0)
    two = lax.broadcasted_iota(jnp.int32, (total, total), 1)
    local = ((one ^ two) & most) == 0
    keep = local & (one != two) & jnp.logical_not(dead)
    best[0] = jnp.maximum(
        jnp.max(jnp.where(keep, gram, -2.0), axis=0, keepdims=True), -1.0
    )

    def back(k):
        peer = me ^ k
        lanes = pl.ds(pl.multiple_of(peer * block // LANES * LANES, LANES), LANES)
        return pltpu.make_async_remote_copy(
            src_ref=best.at[:, :, lanes],
            dst_ref=returned.at[pl.ds(me, 1)],
            send_sem=back_send_sem.at[k],
            recv_sem=back_recv_sem.at[k],
            device_id={"clu": peer},
            device_id_type=pl.DeviceIdType.MESH,
        )

    for k in range(groups - 1, 0, -1):
        back(k).start()
    returned[me] = best[0, :, pl.ds(pl.multiple_of(me * block // LANES * LANES, LANES), LANES)]
    for k in range(1, groups):
        back(k).wait()

    picked = jnp.zeros((count, LANES), jnp.float32)
    for owner in range(groups):
        picked = jnp.where(owner_col == owner, returned[owner], picked)
    lane = lax.broadcasted_iota(jnp.int32, (count, LANES), 1)
    result = jnp.sum(jnp.where(lane == place_col, picked, 0.0), axis=1, keepdims=True)
    out_ref[...] = jnp.sum(jnp.where(row_id == col_id, result, 0.0), axis=0, keepdims=True)


def kernel_shards(embeddings, assignment):
    groups = lax.axis_size("clu")
    count, width = embeddings.shape
    most = 2 * count // (CLU_DEV * groups)
    total = CLU_DEV * groups * most
    out = pl.pallas_call(
        functools.partial(exchange_kernel, groups, most),
        out_shape=jax.ShapeDtypeStruct((1, count), jnp.float32),
        in_specs=[
            pl.BlockSpec(memory_space=pl.ANY),
            pl.BlockSpec(memory_space=pltpu.VMEM),
        ],
        out_specs=pl.BlockSpec(memory_space=pltpu.VMEM),
        scratch_shapes=[
            pltpu.VMEM((count, width), jnp.bfloat16),
            pltpu.VMEM((total, width), jnp.bfloat16),
            pltpu.VMEM((total, width), jnp.bfloat16),
            pltpu.VMEM((1, 1, total), jnp.float32),
            pltpu.VMEM((groups, 1, LANES), jnp.float32),
            pltpu.SemaphoreType.DMA((4,)),
            pltpu.SemaphoreType.DMA((groups,)),
            pltpu.SemaphoreType.DMA((groups,)),
            pltpu.SemaphoreType.DMA((groups,)),
            pltpu.SemaphoreType.DMA((groups,)),
        ],
        compiler_params=pltpu.CompilerParams(collective_id=0, has_side_effects=True),
    )(embeddings, assignment.reshape(1, count))
    return out.reshape(count)


def slot_index(cluster, groups, most):
    count = cluster.shape[0]
    order = jnp.argsort(cluster, stable=True)
    ranked = cluster[order]
    first = jnp.searchsorted(ranked, ranked, side="left")
    rank_sorted = jnp.arange(count, dtype=jnp.int32) - first
    rank = jnp.zeros((count,), jnp.int32).at[order].set(rank_sorted)
    local = cluster % CLU_DEV
    owner = cluster // CLU_DEV
    return (local * groups + owner) * most + rank


def cluster_scores(pieces):
    rows, flags = pieces
    items = rows.shape[0]
    width = rows.shape[1] * rows.shape[2]
    rows = rows.reshape(items, width, rows.shape[3])
    flags = flags.reshape(items, width)
    offsets = jnp.arange(width, dtype=jnp.int32)
    distinct = offsets[:, None] != offsets[None, :]

    def single(pair):
        block, marks = pair
        gram = lax.dot_general(
            block, block, (((1,), (1,)), ((), ())), preferred_element_type=jnp.float32
        )
        keep = distinct & (marks > 0)[None, :]
        best = jnp.max(jnp.where(keep, gram, jnp.float32(-2.0)), axis=1)
        return jnp.maximum(best, jnp.float32(-1.0))

    best = lax.map(single, (rows, flags))
    return best.reshape(items, 1, width)


def general_shards(embeddings, assignment):
    groups = lax.axis_size("clu")
    count = embeddings.shape[0]
    width = embeddings.shape[1]
    most = 2 * count // (CLU_DEV * groups)
    unit = normalize(embeddings)
    cluster = assignment[:, 0]
    slot = slot_index(cluster, groups, most)
    total = CLU_DEV * groups * most
    outgoing = jnp.zeros((total, width), jnp.bfloat16).at[slot].set(unit)
    marks = jnp.zeros((total,), jnp.bfloat16).at[slot].set(jnp.ones((count,), jnp.bfloat16))
    outgoing = outgoing.reshape(CLU_DEV, groups, most, width)
    marks = marks.reshape(CLU_DEV, groups, most)
    arrived = (
        lax.all_to_all(outgoing, "clu", split_axis=1, concat_axis=2, tiled=True),
        lax.all_to_all(marks, "clu", split_axis=1, concat_axis=2, tiled=True),
    )
    best = cluster_scores(arrived)
    returned = lax.all_to_all(best, "clu", split_axis=2, concat_axis=1, tiled=True)
    return returned.reshape(total)[slot]


def shards(embeddings, assignment):
    groups = lax.axis_size("clu")
    count = embeddings.shape[0]
    most = 2 * count // (CLU_DEV * groups)
    block = CLU_DEV * most
    power = groups & (groups - 1) == 0 and most & (most - 1) == 0
    if power and block % 16 == 0 and LANES % block == 0 and (groups * block) % LANES == 0:
        return kernel_shards(embeddings, assignment)
    return general_shards(embeddings, assignment)


def solution(mesh):
    in_specs = (P(("lang", "clu"), None), P(("lang", "clu"), None))
    out_specs = P(("lang", "clu"))
    return jax.shard_map(shards, mesh=mesh, in_specs=in_specs, out_specs=out_specs, check_vma=False)
```

```python
import functools

import jax
import jax.numpy as jnp
from jax import lax
from jax.experimental import pallas as pl
from jax.experimental.pallas import tpu as pltpu
from jax.sharding import PartitionSpec as P

CLU_DEV = 2
LANES = 128
EPS = 1e-06
DEAD = 4.0


def normalize(embeddings):
    values = embeddings.astype(jnp.float32)
    scale = lax.rsqrt(jnp.sum(values * values, axis=-1, keepdims=True) + EPS)
    return (values * scale).astype(jnp.bfloat16)


def exchange_kernel(
    groups, most, emb_ref, cluster_ref, out_ref,
    unit, outgoing, arrived, best, returned,
    load_sem, send_sem, recv_sem, back_send_sem, back_recv_sem,
):
    count, width = unit.shape
    block = CLU_DEV * most
    total = groups * block
    me = lax.axis_index("clu")
    chunks = 4
    step = count // chunks

    def load(c):
        rows = pl.ds(c * step, step)
        return pltpu.make_async_copy(emb_ref.at[rows], unit.at[rows], load_sem.at[c])

    for c in range(chunks):
        load(c).start()

    barrier = pltpu.get_barrier_semaphore()
    for k in range(1, groups):
        pl.semaphore_signal(
            barrier, inc=1, device_id={"clu": me ^ k}, device_id_type=pl.DeviceIdType.MESH
        )

    cluster_row = cluster_ref[...]
    row_id = lax.broadcasted_iota(jnp.int32, (count, count), 0)
    col_id = lax.broadcasted_iota(jnp.int32, (count, count), 1)
    spread = jnp.broadcast_to(cluster_row, (count, count))
    cluster_col = jnp.sum(jnp.where(row_id == col_id, spread, 0), axis=1, keepdims=True)
    same = cluster_col == spread
    rank_row = jnp.sum(jnp.where(same & (row_id < col_id), 1, 0), axis=0, keepdims=True)
    slot_row = cluster_row * most + rank_row
    slot_id = lax.broadcasted_iota(jnp.int32, (total, count), 0)
    hit = slot_id == jnp.broadcast_to(slot_row, (total, count))
    place = jnp.where(hit, 1.0, 0.0)
    live = jnp.max(place, axis=1, keepdims=True)
    place = place.astype(jnp.bfloat16)

    for c in range(chunks):
        load(c).wait()
        rows = pl.ds(c * step, step)
        unit[rows, :] = normalize(unit[rows, :])

    outgoing[...] = jnp.dot(
        place, unit[...], preferred_element_type=jnp.float32
    ).astype(jnp.bfloat16)
    lane = lax.broadcasted_iota(jnp.int32, (total, LANES), 1)
    head = outgoing[:, 0:LANES].astype(jnp.float32)
    outgoing[:, 0:LANES] = jnp.where(
        (lane == 0) & (live < 0.5), DEAD, head
    ).astype(jnp.bfloat16)

    pl.semaphore_wait(barrier, groups - 1)

    mine = pl.ds(pl.multiple_of(me * block, block), block)

    def send(k):
        peer = me ^ k
        return pltpu.make_async_remote_copy(
            src_ref=outgoing.at[pl.ds(pl.multiple_of(peer * block, block), block)],
            dst_ref=arrived.at[mine],
            send_sem=send_sem.at[k],
            recv_sem=recv_sem.at[k],
            device_id={"clu": peer},
            device_id_type=pl.DeviceIdType.MESH,
        )

    for k in range(1, groups):
        send(k).start()
    arrived[mine, :] = outgoing[mine, :]

    rank_col = jnp.sum(
        jnp.where(same & (col_id < row_id), 1, 0), axis=1, keepdims=True
    )
    owner_col = cluster_col // CLU_DEV
    place_col = (cluster_col % CLU_DEV) * most + rank_col + (me * block) % LANES

    for k in range(1, groups):
        send(k).wait()

    rows = arrived[...]
    gram = lax.dot_general(
        rows, rows, (((1,), (1,)), ((), ())), preferred_element_type=jnp.float32
    )
    dead = rows[:, 0:1].astype(jnp.float32) > 2.0
    one = lax.broadcasted_iota(jnp.int32, (total, total), 0)
    two = lax.broadcasted_iota(jnp.int32, (total, total), 1)
    local = ((one ^ two) & most) == 0
    keep = local & (one != two) & jnp.logical_not(dead)
    best[0] = jnp.maximum(
        jnp.max(jnp.where(keep, gram, -2.0), axis=0, keepdims=True), -1.0
    )

    def back(k):
        peer = me ^ k
        lanes = pl.ds(pl.multiple_of(peer * block // LANES * LANES, LANES), LANES)
        return pltpu.make_async_remote_copy(
            src_ref=best.at[:, :, lanes],
            dst_ref=returned.at[pl.ds(me, 1)],
            send_sem=back_send_sem.at[k],
            recv_sem=back_recv_sem.at[k],
            device_id={"clu": peer},
            device_id_type=pl.DeviceIdType.MESH,
        )

    for k in range(groups - 1, 0, -1):
        back(k).start()
    returned[me] = best[0, :, pl.ds(pl.multiple_of(me * block // LANES * LANES, LANES), LANES)]
    for k in range(1, groups):
        back(k).wait()

    picked = jnp.zeros((count, LANES), jnp.float32)
    for owner in range(groups):
        picked = jnp.where(owner_col == owner, returned[owner], picked)
    lane = lax.broadcasted_iota(jnp.int32, (count, LANES), 1)
    result = jnp.sum(jnp.where(lane == place_col, picked, 0.0), axis=1, keepdims=True)
    out_ref[...] = jnp.sum(jnp.where(row_id == col_id, result, 0.0), axis=0, keepdims=True)


def kernel_shards(embeddings, assignment):
    groups = lax.axis_size("clu")
    count, width = embeddings.shape
    most = 2 * count // (CLU_DEV * groups)
    total = CLU_DEV * groups * most
    out = pl.pallas_call(
        functools.partial(exchange_kernel, groups, most),
        out_shape=jax.ShapeDtypeStruct((1, count), jnp.float32),
        in_specs=[
            pl.BlockSpec(memory_space=pl.ANY),
            pl.BlockSpec(memory_space=pltpu.VMEM),
        ],
        out_specs=pl.BlockSpec(memory_space=pltpu.VMEM),
        scratch_shapes=[
            pltpu.VMEM((count, width), jnp.bfloat16),
            pltpu.VMEM((total, width), jnp.bfloat16),
            pltpu.VMEM((total, width), jnp.bfloat16),
            pltpu.VMEM((1, 1, total), jnp.float32),
            pltpu.VMEM((groups, 1, LANES), jnp.float32),
            pltpu.SemaphoreType.DMA((4,)),
            pltpu.SemaphoreType.DMA((groups,)),
            pltpu.SemaphoreType.DMA((groups,)),
            pltpu.SemaphoreType.DMA((groups,)),
            pltpu.SemaphoreType.DMA((groups,)),
        ],
        compiler_params=pltpu.CompilerParams(collective_id=0, has_side_effects=True),
    )(embeddings, assignment.reshape(1, count))
    return out.reshape(count)


def slot_index(cluster, groups, most):
    count = cluster.shape[0]
    order = jnp.argsort(cluster, stable=True)
    ranked = cluster[order]
    first = jnp.searchsorted(ranked, ranked, side="left")
    rank_sorted = jnp.arange(count, dtype=jnp.int32) - first
    rank = jnp.zeros((count,), jnp.int32).at[order].set(rank_sorted)
    local = cluster % CLU_DEV
    owner = cluster // CLU_DEV
    return (local * groups + owner) * most + rank


def cluster_scores(pieces):
    rows, flags = pieces
    items = rows.shape[0]
    width = rows.shape[1] * rows.shape[2]
    rows = rows.reshape(items, width, rows.shape[3])
    flags = flags.reshape(items, width)
    offsets = jnp.arange(width, dtype=jnp.int32)
    distinct = offsets[:, None] != offsets[None, :]

    def single(pair):
        block, marks = pair
        gram = lax.dot_general(
            block, block, (((1,), (1,)), ((), ())), preferred_element_type=jnp.float32
        )
        keep = distinct & (marks > 0)[None, :]
        best = jnp.max(jnp.where(keep, gram, jnp.float32(-2.0)), axis=1)
        return jnp.maximum(best, jnp.float32(-1.0))

    best = lax.map(single, (rows, flags))
    return best.reshape(items, 1, width)


def general_shards(embeddings, assignment):
    groups = lax.axis_size("clu")
    count = embeddings.shape[0]
    width = embeddings.shape[1]
    most = 2 * count // (CLU_DEV * groups)
    unit = normalize(embeddings)
    cluster = assignment[:, 0]
    slot = slot_index(cluster, groups, most)
    total = CLU_DEV * groups * most
    outgoing = jnp.zeros((total, width), jnp.bfloat16).at[slot].set(unit)
    marks = jnp.zeros((total,), jnp.bfloat16).at[slot].set(jnp.ones((count,), jnp.bfloat16))
    outgoing = outgoing.reshape(CLU_DEV, groups, most, width)
    marks = marks.reshape(CLU_DEV, groups, most)
    arrived = (
        lax.all_to_all(outgoing, "clu", split_axis=1, concat_axis=2, tiled=True),
        lax.all_to_all(marks, "clu", split_axis=1, concat_axis=2, tiled=True),
    )
    best = cluster_scores(arrived)
    returned = lax.all_to_all(best, "clu", split_axis=2, concat_axis=1, tiled=True)
    return returned.reshape(total)[slot]


def shards(embeddings, assignment):
    groups = lax.axis_size("clu")
    count = embeddings.shape[0]
    most = 2 * count // (CLU_DEV * groups)
    block = CLU_DEV * most
    power = groups & (groups - 1) == 0 and most & (most - 1) == 0
    if power and block % 16 == 0 and LANES % block == 0 and (groups * block) % LANES == 0:
        return kernel_shards(embeddings, assignment)
    return general_shards(embeddings, assignment)


def solution(mesh):
    in_specs = (P(("lang", "clu"), None), P(("lang", "clu"), None))
    out_specs = P(("lang", "clu"))
    return jax.shard_map(shards, mesh=mesh, in_specs=in_specs, out_specs=out_specs, check_vma=False)
```

```python
import functools

import jax
import jax.numpy as jnp
from jax import lax
from jax.experimental import pallas as pl
from jax.experimental.pallas import tpu as pltpu
from jax.sharding import PartitionSpec as P

CLU_DEV = 2
LANES = 128
EPS = 1e-06
DEAD = 4.0


def normalize(embeddings):
    values = embeddings.astype(jnp.float32)
    scale = lax.rsqrt(jnp.sum(values * values, axis=-1, keepdims=True) + EPS)
    return (values * scale).astype(jnp.bfloat16)


def exchange_kernel(
    groups, most, emb_ref, cluster_ref, out_ref,
    unit, outgoing, arrived, best, returned,
    load_sem, send_sem, recv_sem, back_send_sem, back_recv_sem,
):
    count, width = unit.shape
    block = CLU_DEV * most
    total = groups * block
    batch = LANES // block
    me = lax.axis_index("clu")
    chunks = 4
    step = count // chunks

    def load(c):
        rows = pl.ds(c * step, step)
        return pltpu.make_async_copy(emb_ref.at[rows], unit.at[rows], load_sem.at[c])

    for c in range(chunks):
        load(c).start()

    barrier = pltpu.get_barrier_semaphore()
    for k in range(1, groups):
        pl.semaphore_signal(
            barrier, inc=1, device_id={"clu": me ^ k}, device_id_type=pl.DeviceIdType.MESH
        )

    def slot_of(cluster, rank):
        peer = (cluster // CLU_DEV) ^ me
        return peer * block + (cluster % CLU_DEV) * most + rank

    cluster_row = cluster_ref[...]
    row_id = lax.broadcasted_iota(jnp.int32, (count, count), 0)
    col_id = lax.broadcasted_iota(jnp.int32, (count, count), 1)
    spread = jnp.broadcast_to(cluster_row, (count, count))
    cluster_col = jnp.sum(jnp.where(row_id == col_id, spread, 0), axis=1, keepdims=True)
    same = cluster_col == spread
    rank_row = jnp.sum(jnp.where(same & (row_id < col_id), 1, 0), axis=0, keepdims=True)
    slot_row = jnp.broadcast_to(slot_of(cluster_row, rank_row), (LANES, count))

    for c in range(chunks):
        load(c).wait()
        rows = pl.ds(c * step, step)
        unit[rows, :] = normalize(unit[rows, :])

    def send(k):
        rows = pl.ds(k * block, block)
        return pltpu.make_async_remote_copy(
            src_ref=outgoing.at[rows],
            dst_ref=arrived.at[rows],
            send_sem=send_sem.at[k],
            recv_sem=recv_sem.at[k],
            device_id={"clu": me ^ k},
            device_id_type=pl.DeviceIdType.MESH,
        )

    first = lax.broadcasted_iota(jnp.int32, (count, LANES), 1) == 0
    mark = jnp.where(first, DEAD, 0.0).astype(jnp.bfloat16)
    blank = jnp.where(
        lax.broadcasted_iota(jnp.int32, (LANES, LANES), 1) == 0, DEAD, 0.0
    )
    for g in range(groups // batch):
        rows = pl.ds(g * LANES, LANES)
        hit = lax.broadcasted_iota(jnp.int32, (LANES, count), 0) + g * LANES == slot_row
        place = jnp.where(hit, 1.0, 0.0).astype(jnp.bfloat16)
        packed = jnp.dot(place, unit[...], preferred_element_type=jnp.float32)
        used = jnp.dot(place, mark, preferred_element_type=jnp.float32)
        outgoing[rows, :] = packed.astype(jnp.bfloat16)
        outgoing[rows, 0:LANES] = (packed[:, 0:LANES] + (blank - used)).astype(jnp.bfloat16)
        if g == 0:
            pl.semaphore_wait(barrier, groups - 1)
        for k in range(max(1, g * batch), (g + 1) * batch):
            send(k).start()
    arrived[0:block, :] = outgoing[0:block, :]

    rank_col = jnp.sum(
        jnp.where(same & (col_id < row_id), 1, 0), axis=1, keepdims=True
    )
    slot_col = slot_of(cluster_col, rank_col)
    peer_col = slot_col // block
    chosen = lax.broadcasted_iota(jnp.int32, (count, LANES), 1) == slot_col % LANES

    def scores(one, two):
        left, right = arrived[one[0] : one[1], :], arrived[two[0] : two[1], :]
        gram = lax.dot_general(
            left, right, (((1,), (1,)), ((), ())), preferred_element_type=jnp.float32
        )
        dead = left[:, 0:1].astype(jnp.float32) > 2.0
        this = lax.broadcasted_iota(jnp.int32, gram.shape, 0) + one[0]
        other = lax.broadcasted_iota(jnp.int32, gram.shape, 1) + two[0]
        keep = (((this ^ other) & most) == 0) & (this != other) & jnp.logical_not(dead)
        return jnp.max(jnp.where(keep, gram, -1.0), axis=0, keepdims=True)

    for g in range(groups // batch):
        low, high = g * LANES, (g + 1) * LANES
        for k in range(max(1, g * batch), (g + 1) * batch):
            send(k).wait_recv()
        if g:
            best[0, :, 0:low] = jnp.maximum(best[0, :, 0:low], scores((low, high), (0, low)))
        best[0, :, low:high] = jnp.maximum(scores((0, high), (low, high)), -1.0)

    def back(k):
        return pltpu.make_async_remote_copy(
            src_ref=best.at[:, :, pl.ds(k // batch * LANES, LANES)],
            dst_ref=returned.at[pl.ds(k, 1)],
            send_sem=back_send_sem.at[k],
            recv_sem=back_recv_sem.at[k],
            device_id={"clu": me ^ k},
            device_id_type=pl.DeviceIdType.MESH,
        )

    for k in range(groups - 1, 0, -1):
        back(k).start()
    returned[0] = best[0, :, 0:LANES]
    for k in range(1, groups):
        send(k).wait_send()
    for k in range(1, groups):
        back(k).wait()

    picked = jnp.zeros((count, LANES), jnp.float32)
    for k in range(groups):
        picked = jnp.where(peer_col == k, returned[k], picked)
    result = jnp.sum(jnp.where(chosen, picked, 0.0), axis=1, keepdims=True)
    result = jnp.sum(jnp.where(row_id == col_id, result, 0.0), axis=0, keepdims=True)
    out_ref[...] = result.reshape(out_ref.shape)


def kernel_shards(embeddings, assignment):
    groups = lax.axis_size("clu")
    count, width = embeddings.shape
    most = 2 * count // (CLU_DEV * groups)
    total = CLU_DEV * groups * most
    return pl.pallas_call(
        functools.partial(exchange_kernel, groups, most),
        out_shape=jax.ShapeDtypeStruct((count,), jnp.float32),
        in_specs=[
            pl.BlockSpec(memory_space=pl.ANY),
            pl.BlockSpec(memory_space=pltpu.VMEM),
        ],
        out_specs=pl.BlockSpec(memory_space=pltpu.VMEM),
        scratch_shapes=[
            pltpu.VMEM((count, width), jnp.bfloat16),
            pltpu.VMEM((total, width), jnp.bfloat16),
            pltpu.VMEM((total, width), jnp.bfloat16),
            pltpu.VMEM((1, 1, total), jnp.float32),
            pltpu.VMEM((groups, 1, LANES), jnp.float32),
            pltpu.SemaphoreType.DMA((4,)),
            pltpu.SemaphoreType.DMA((groups,)),
            pltpu.SemaphoreType.DMA((groups,)),
            pltpu.SemaphoreType.DMA((groups,)),
            pltpu.SemaphoreType.DMA((groups,)),
        ],
        compiler_params=pltpu.CompilerParams(collective_id=0, has_side_effects=True),
    )(embeddings, assignment.reshape(1, count))


def slot_index(cluster, groups, most):
    count = cluster.shape[0]
    order = jnp.argsort(cluster, stable=True)
    ranked = cluster[order]
    first = jnp.searchsorted(ranked, ranked, side="left")
    rank_sorted = jnp.arange(count, dtype=jnp.int32) - first
    rank = jnp.zeros((count,), jnp.int32).at[order].set(rank_sorted)
    local = cluster % CLU_DEV
    owner = cluster // CLU_DEV
    return (local * groups + owner) * most + rank


def cluster_scores(pieces):
    rows, flags = pieces
    items = rows.shape[0]
    width = rows.shape[1] * rows.shape[2]
    rows = rows.reshape(items, width, rows.shape[3])
    flags = flags.reshape(items, width)
    offsets = jnp.arange(width, dtype=jnp.int32)
    distinct = offsets[:, None] != offsets[None, :]

    def single(pair):
        block, marks = pair
        gram = lax.dot_general(
            block, block, (((1,), (1,)), ((), ())), preferred_element_type=jnp.float32
        )
        keep = distinct & (marks > 0)[None, :]
        best = jnp.max(jnp.where(keep, gram, jnp.float32(-2.0)), axis=1)
        return jnp.maximum(best, jnp.float32(-1.0))

    best = lax.map(single, (rows, flags))
    return best.reshape(items, 1, width)


def general_shards(embeddings, assignment):
    groups = lax.axis_size("clu")
    count = embeddings.shape[0]
    width = embeddings.shape[1]
    most = 2 * count // (CLU_DEV * groups)
    unit = normalize(embeddings)
    cluster = assignment[:, 0]
    slot = slot_index(cluster, groups, most)
    total = CLU_DEV * groups * most
    outgoing = jnp.zeros((total, width), jnp.bfloat16).at[slot].set(unit)
    marks = jnp.zeros((total,), jnp.bfloat16).at[slot].set(jnp.ones((count,), jnp.bfloat16))
    outgoing = outgoing.reshape(CLU_DEV, groups, most, width)
    marks = marks.reshape(CLU_DEV, groups, most)
    arrived = (
        lax.all_to_all(outgoing, "clu", split_axis=1, concat_axis=2, tiled=True),
        lax.all_to_all(marks, "clu", split_axis=1, concat_axis=2, tiled=True),
    )
    best = cluster_scores(arrived)
    returned = lax.all_to_all(best, "clu", split_axis=2, concat_axis=1, tiled=True)
    return returned.reshape(total)[slot]


def shards(embeddings, assignment):
    groups = lax.axis_size("clu")
    count = embeddings.shape[0]
    most = 2 * count // (CLU_DEV * groups)
    block = CLU_DEV * most
    power = groups & (groups - 1) == 0 and most & (most - 1) == 0
    if power and block % 16 == 0 and LANES % block == 0 and (groups * block) % LANES == 0:
        return kernel_shards(embeddings, assignment)
    return general_shards(embeddings, assignment)


def solution(mesh):
    in_specs = (P(("lang", "clu"), None), P(("lang", "clu"), None))
    out_specs = P(("lang", "clu"))
    return jax.shard_map(shards, mesh=mesh, in_specs=in_specs, out_specs=out_specs, check_vma=False)
```

```python
import functools

import jax
import jax.numpy as jnp
from jax import lax
from jax.experimental import pallas as pl
from jax.experimental.pallas import tpu as pltpu
from jax.sharding import PartitionSpec as P

CLU_DEV = 2
LANES = 128
EPS = 1e-06
DEAD = 4.0


def normalize(embeddings):
    values = embeddings.astype(jnp.float32)
    scale = lax.rsqrt(jnp.sum(values * values, axis=-1, keepdims=True) + EPS)
    return (values * scale).astype(jnp.bfloat16)


def exchange_kernel(
    groups, most, emb_ref, cluster_ref, out_ref,
    unit, outgoing, arrived, best, returned,
    load_sem, send_sem, recv_sem, back_send_sem, back_recv_sem, ready,
):
    count, width = unit.shape
    block = CLU_DEV * most
    total = groups * block
    batch = LANES // block
    me = lax.axis_index("clu")
    chunks = 4
    step = count // chunks

    def load(c):
        rows = pl.ds(c * step, step)
        return pltpu.make_async_copy(emb_ref.at[rows], unit.at[rows], load_sem.at[c])

    for c in range(chunks):
        load(c).start()

    barrier = pltpu.get_barrier_semaphore()
    bits = groups.bit_length() - 1
    for b in range(bits):
        pl.semaphore_signal(
            barrier, inc=1, device_id={"clu": me ^ (1 << b)},
            device_id_type=pl.DeviceIdType.MESH,
        )

    def tell(stage):
        for b in range(bits):
            pl.semaphore_signal(
                ready.at[stage, b], inc=1, device_id={"clu": me ^ (1 << b)},
                device_id_type=pl.DeviceIdType.MESH,
            )

    def hear(stage):
        for b in range(bits):
            pl.semaphore_wait(ready.at[stage, b], 1)

    def slot_of(cluster, rank):
        peer = (cluster // CLU_DEV) ^ me
        return peer * block + (cluster % CLU_DEV) * most + rank

    cluster_row = cluster_ref[...]
    row_id = lax.broadcasted_iota(jnp.int32, (count, count), 0)
    col_id = lax.broadcasted_iota(jnp.int32, (count, count), 1)
    spread = jnp.broadcast_to(cluster_row, (count, count))
    cluster_col = jnp.sum(jnp.where(row_id == col_id, spread, 0), axis=1, keepdims=True)
    same = cluster_col == spread
    rank_row = jnp.sum(jnp.where(same & (row_id < col_id), 1, 0), axis=0, keepdims=True)
    slot_row = jnp.broadcast_to(slot_of(cluster_row, rank_row), (LANES, count))

    for c in range(chunks):
        load(c).wait()
        rows = pl.ds(c * step, step)
        unit[rows, :] = normalize(unit[rows, :])

    def send(k):
        rows = pl.ds(pl.multiple_of(k * block, block), block)
        return pltpu.make_async_remote_copy(
            src_ref=outgoing.at[rows],
            dst_ref=arrived.at[rows],
            send_sem=send_sem.at[k],
            recv_sem=recv_sem.at[k],
            device_id={"clu": me ^ k},
            device_id_type=pl.DeviceIdType.MESH,
        )

    first = lax.broadcasted_iota(jnp.int32, (count, LANES), 1) == 0
    mark = jnp.where(first, DEAD, 0.0).astype(jnp.bfloat16)
    blank = jnp.where(
        lax.broadcasted_iota(jnp.int32, (LANES, LANES), 1) == 0, DEAD, 0.0
    )
    pl.semaphore_wait(barrier, bits)
    tell(0)
    for g in reversed(range(groups // batch)):
        rows = pl.ds(g * LANES, LANES)
        hit = lax.broadcasted_iota(jnp.int32, (LANES, count), 0) + g * LANES == slot_row
        place = jnp.where(hit, 1.0, 0.0).astype(jnp.bfloat16)
        packed = jnp.dot(place, unit[...], preferred_element_type=jnp.float32)
        used = jnp.dot(place, mark, preferred_element_type=jnp.float32)
        outgoing[rows, :] = packed.astype(jnp.bfloat16)
        outgoing[rows, 0:LANES] = (packed[:, 0:LANES] + (blank - used)).astype(jnp.bfloat16)
    for n in range(1, bits + 1):
        if n > 1:
            hear(n - 2)
            if n < bits:
                tell(n - 1)
        for k in reversed(range(1, groups)):
            if k.bit_count() == n:
                send(k).start()
    arrived[0:block, :] = outgoing[0:block, :]

    rank_col = jnp.sum(
        jnp.where(same & (col_id < row_id), 1, 0), axis=1, keepdims=True
    )
    slot_col = slot_of(cluster_col, rank_col)
    peer_col = slot_col // block
    chosen = lax.broadcasted_iota(jnp.int32, (count, LANES), 1) == slot_col % LANES

    def scores(one, two):
        left, right = arrived[one[0] : one[1], :], arrived[two[0] : two[1], :]
        gram = lax.dot_general(
            left, right, (((1,), (1,)), ((), ())), preferred_element_type=jnp.float32
        )
        dead = left[:, 0:1].astype(jnp.float32) > 2.0
        this = lax.broadcasted_iota(jnp.int32, gram.shape, 0) + one[0]
        other = lax.broadcasted_iota(jnp.int32, gram.shape, 1) + two[0]
        keep = (((this ^ other) & most) == 0) & (this != other) & jnp.logical_not(dead)
        return jnp.max(jnp.where(keep, gram, -1.0), axis=0, keepdims=True)

    for g in range(groups // batch):
        low, high = g * LANES, (g + 1) * LANES
        for k in range(max(1, g * batch), (g + 1) * batch):
            send(k).wait_recv()
        if g:
            best[0, :, 0:low] = jnp.maximum(best[0, :, 0:low], scores((low, high), (0, low)))
        best[0, :, low:high] = jnp.maximum(scores((0, high), (low, high)), -1.0)

    def back(k):
        return pltpu.make_async_remote_copy(
            src_ref=best.at[:, :, pl.ds(k // batch * LANES, LANES)],
            dst_ref=returned.at[pl.ds(k, 1)],
            send_sem=back_send_sem.at[k],
            recv_sem=back_recv_sem.at[k],
            device_id={"clu": me ^ k},
            device_id_type=pl.DeviceIdType.MESH,
        )

    for k in range(groups - 1, 0, -1):
        back(k).start()
    returned[0] = best[0, :, 0:LANES]
    for k in range(1, groups):
        send(k).wait_send()
    picked = jnp.broadcast_to(returned[0], (count, LANES))
    for k in range(1, groups):
        back(k).wait_recv()
        picked = jnp.where(peer_col == k, returned[k], picked)
    for k in range(1, groups):
        back(k).wait_send()
    result = jnp.sum(jnp.where(chosen, picked, 0.0), axis=1, keepdims=True)
    result = jnp.sum(jnp.where(row_id == col_id, result, 0.0), axis=0, keepdims=True)
    out_ref[...] = result.reshape(out_ref.shape)


def kernel_shards(embeddings, assignment):
    groups = lax.axis_size("clu")
    count, width = embeddings.shape
    most = 2 * count // (CLU_DEV * groups)
    total = CLU_DEV * groups * most
    return pl.pallas_call(
        functools.partial(exchange_kernel, groups, most),
        out_shape=jax.ShapeDtypeStruct((count,), jnp.float32),
        in_specs=[
            pl.BlockSpec(memory_space=pl.ANY),
            pl.BlockSpec(memory_space=pltpu.VMEM),
        ],
        out_specs=pl.BlockSpec(memory_space=pltpu.VMEM),
        scratch_shapes=[
            pltpu.VMEM((count, width), jnp.bfloat16),
            pltpu.VMEM((total, width), jnp.bfloat16),
            pltpu.VMEM((total, width), jnp.bfloat16),
            pltpu.VMEM((1, 1, total), jnp.float32),
            pltpu.VMEM((groups, 1, LANES), jnp.float32),
            pltpu.SemaphoreType.DMA((4,)),
            pltpu.SemaphoreType.DMA((groups,)),
            pltpu.SemaphoreType.DMA((groups,)),
            pltpu.SemaphoreType.DMA((groups,)),
            pltpu.SemaphoreType.DMA((groups,)),
            pltpu.SemaphoreType.REGULAR((groups.bit_length(), groups.bit_length())),
        ],
        compiler_params=pltpu.CompilerParams(collective_id=0, has_side_effects=True),
    )(embeddings, assignment.reshape(1, count))


def slot_index(cluster, groups, most):
    count = cluster.shape[0]
    order = jnp.argsort(cluster, stable=True)
    ranked = cluster[order]
    first = jnp.searchsorted(ranked, ranked, side="left")
    rank_sorted = jnp.arange(count, dtype=jnp.int32) - first
    rank = jnp.zeros((count,), jnp.int32).at[order].set(rank_sorted)
    local = cluster % CLU_DEV
    owner = cluster // CLU_DEV
    return (local * groups + owner) * most + rank


def cluster_scores(pieces):
    rows, flags = pieces
    items = rows.shape[0]
    width = rows.shape[1] * rows.shape[2]
    rows = rows.reshape(items, width, rows.shape[3])
    flags = flags.reshape(items, width)
    offsets = jnp.arange(width, dtype=jnp.int32)
    distinct = offsets[:, None] != offsets[None, :]

    def single(pair):
        block, marks = pair
        gram = lax.dot_general(
            block, block, (((1,), (1,)), ((), ())), preferred_element_type=jnp.float32
        )
        keep = distinct & (marks > 0)[None, :]
        best = jnp.max(jnp.where(keep, gram, jnp.float32(-2.0)), axis=1)
        return jnp.maximum(best, jnp.float32(-1.0))

    best = lax.map(single, (rows, flags))
    return best.reshape(items, 1, width)


def general_shards(embeddings, assignment):
    groups = lax.axis_size("clu")
    count = embeddings.shape[0]
    width = embeddings.shape[1]
    most = 2 * count // (CLU_DEV * groups)
    unit = normalize(embeddings)
    cluster = assignment[:, 0]
    slot = slot_index(cluster, groups, most)
    total = CLU_DEV * groups * most
    outgoing = jnp.zeros((total, width), jnp.bfloat16).at[slot].set(unit)
    marks = jnp.zeros((total,), jnp.bfloat16).at[slot].set(jnp.ones((count,), jnp.bfloat16))
    outgoing = outgoing.reshape(CLU_DEV, groups, most, width)
    marks = marks.reshape(CLU_DEV, groups, most)
    arrived = (
        lax.all_to_all(outgoing, "clu", split_axis=1, concat_axis=2, tiled=True),
        lax.all_to_all(marks, "clu", split_axis=1, concat_axis=2, tiled=True),
    )
    best = cluster_scores(arrived)
    returned = lax.all_to_all(best, "clu", split_axis=2, concat_axis=1, tiled=True)
    return returned.reshape(total)[slot]


def shards(embeddings, assignment):
    groups = lax.axis_size("clu")
    count = embeddings.shape[0]
    most = 2 * count // (CLU_DEV * groups)
    block = CLU_DEV * most
    power = groups & (groups - 1) == 0 and most & (most - 1) == 0
    if power and block % 16 == 0 and LANES % block == 0 and (groups * block) % LANES == 0:
        return kernel_shards(embeddings, assignment)
    return general_shards(embeddings, assignment)


def solution(mesh):
    in_specs = (P(("lang", "clu"), None), P(("lang", "clu"), None))
    out_specs = P(("lang", "clu"))
    return jax.shard_map(shards, mesh=mesh, in_specs=in_specs, out_specs=out_specs, check_vma=False)
```

```python
import functools

import jax
import jax.numpy as jnp
from jax import lax
from jax.experimental import pallas as pl
from jax.experimental.pallas import tpu as pltpu
from jax.sharding import PartitionSpec as P

CLU_DEV = 2
LANES = 128
EPS = 1e-06
DEAD = 4.0


def normalize(embeddings):
    values = embeddings.astype(jnp.float32)
    scale = lax.rsqrt(jnp.sum(values * values, axis=-1, keepdims=True) + EPS)
    return (values * scale).astype(jnp.bfloat16)


def exchange_kernel(
    groups, most, emb_ref, cluster_ref, out_ref,
    unit, outgoing, arrived, best, returned,
    load_sem, send_sem, recv_sem, back_send_sem, back_recv_sem, ready,
):
    count, width = unit.shape
    block = CLU_DEV * most
    total = groups * block
    batch = LANES // block
    me = lax.axis_index("clu")
    chunks = 4
    step = count // chunks

    def load(c):
        rows = pl.ds(c * step, step)
        return pltpu.make_async_copy(emb_ref.at[rows], unit.at[rows], load_sem.at[c])

    for c in range(chunks):
        load(c).start()

    barrier = pltpu.get_barrier_semaphore()
    bits = groups.bit_length() - 1
    for b in range(bits):
        pl.semaphore_signal(
            barrier, inc=1, device_id={"clu": me ^ (1 << b)},
            device_id_type=pl.DeviceIdType.MESH,
        )

    def tell(stage):
        for b in range(bits):
            pl.semaphore_signal(
                ready.at[stage, b], inc=1, device_id={"clu": me ^ (1 << b)},
                device_id_type=pl.DeviceIdType.MESH,
            )

    def hear(stage):
        for b in range(bits):
            pl.semaphore_wait(ready.at[stage, b], 1)

    def slot_of(cluster, rank):
        peer = (cluster // CLU_DEV) ^ me
        return peer * block + (cluster % CLU_DEV) * most + rank

    cluster_row = cluster_ref[...]
    row_id = lax.broadcasted_iota(jnp.int32, (count, count), 0)
    col_id = lax.broadcasted_iota(jnp.int32, (count, count), 1)
    spread = jnp.broadcast_to(cluster_row, (count, count))
    cluster_col = jnp.sum(jnp.where(row_id == col_id, spread, 0), axis=1, keepdims=True)
    same = cluster_col == spread
    rank_row = jnp.sum(jnp.where(same & (row_id < col_id), 1, 0), axis=0, keepdims=True)
    slot_row = jnp.broadcast_to(slot_of(cluster_row, rank_row), (LANES, count))

    for c in range(chunks):
        load(c).wait()
        rows = pl.ds(c * step, step)
        unit[rows, :] = normalize(unit[rows, :])

    def send(k):
        rows = pl.ds(pl.multiple_of(k * block, block), block)
        return pltpu.make_async_remote_copy(
            src_ref=outgoing.at[rows],
            dst_ref=arrived.at[rows],
            send_sem=send_sem.at[k],
            recv_sem=recv_sem.at[k],
            device_id={"clu": me ^ k},
            device_id_type=pl.DeviceIdType.MESH,
        )

    first = lax.broadcasted_iota(jnp.int32, (count, LANES), 1) == 0
    mark = jnp.where(first, DEAD, 0.0).astype(jnp.bfloat16)
    blank = jnp.where(
        lax.broadcasted_iota(jnp.int32, (LANES, LANES), 1) == 0, DEAD, 0.0
    )
    pl.semaphore_wait(barrier, bits)
    tell(0)
    last = groups // batch - 1
    order = sorted(range(groups // batch), key=lambda g: (g == last, -g))
    for g in order:
        rows = pl.ds(g * LANES, LANES)
        hit = lax.broadcasted_iota(jnp.int32, (LANES, count), 0) + g * LANES == slot_row
        place = jnp.where(hit, 1.0, 0.0).astype(jnp.bfloat16)
        packed = jnp.dot(place, unit[...], preferred_element_type=jnp.float32)
        used = jnp.dot(place, mark, preferred_element_type=jnp.float32)
        outgoing[rows, :] = packed.astype(jnp.bfloat16)
        outgoing[rows, 0:LANES] = (packed[:, 0:LANES] + (blank - used)).astype(jnp.bfloat16)
        for k in range(max(1, g * batch), (g + 1) * batch):
            if k.bit_count() == 1:
                send(k).start()
    for n in range(1, bits + 1):
        if n > 1:
            hear(n - 2)
            if n < bits:
                tell(n - 1)
        for k in reversed(range(1, groups)):
            if k.bit_count() == n and n > 1:
                send(k).start()
    arrived[0:block, :] = outgoing[0:block, :]
    best[0] = jnp.full((1, total), -1.0, jnp.float32)

    rank_col = jnp.sum(
        jnp.where(same & (col_id < row_id), 1, 0), axis=1, keepdims=True
    )
    slot_col = slot_of(cluster_col, rank_col)
    peer_col = slot_col // block
    chosen = lax.broadcasted_iota(jnp.int32, (count, LANES), 1) == slot_col % LANES

    def scores(one, two):
        left, right = arrived[one[0] : one[1], :], arrived[two[0] : two[1], :]
        gram = lax.dot_general(
            left, right, (((1,), (1,)), ((), ())), preferred_element_type=jnp.float32
        )
        dead = left[:, 0:1].astype(jnp.float32) > 2.0
        this = lax.broadcasted_iota(jnp.int32, gram.shape, 0) + one[0]
        other = lax.broadcasted_iota(jnp.int32, gram.shape, 1) + two[0]
        keep = (((this ^ other) & most) == 0) & (this != other) & jnp.logical_not(dead)
        return jnp.max(jnp.where(keep, gram, -1.0), axis=0, keepdims=True)

    for g in range(groups // batch):
        low, high = g * LANES, (g + 1) * LANES
        for k in range(max(1, g * batch), (g + 1) * batch):
            send(k).wait_recv()
        best[0, :, 0:high] = jnp.maximum(
            best[0, :, 0:high], scores((low, high), (0, high))
        )
        if g:
            best[0, :, low:high] = jnp.maximum(
                best[0, :, low:high], scores((0, low), (low, high))
            )

    def back(k):
        return pltpu.make_async_remote_copy(
            src_ref=best.at[:, :, pl.ds(k // batch * LANES, LANES)],
            dst_ref=returned.at[pl.ds(k, 1)],
            send_sem=back_send_sem.at[k],
            recv_sem=back_recv_sem.at[k],
            device_id={"clu": me ^ k},
            device_id_type=pl.DeviceIdType.MESH,
        )

    for k in range(groups - 1, 0, -1):
        back(k).start()
    returned[0] = best[0, :, 0:LANES]
    for k in range(1, groups):
        send(k).wait_send()
    picked = jnp.broadcast_to(returned[0], (count, LANES))
    for k in range(1, groups):
        back(k).wait_recv()
        picked = jnp.where(peer_col == k, returned[k], picked)
    for k in range(1, groups):
        back(k).wait_send()
    result = jnp.sum(jnp.where(chosen, picked, 0.0), axis=1, keepdims=True)
    result = jnp.sum(jnp.where(row_id == col_id, result, 0.0), axis=0, keepdims=True)
    out_ref[...] = result.reshape(out_ref.shape)


def kernel_shards(embeddings, assignment):
    groups = lax.axis_size("clu")
    count, width = embeddings.shape
    most = 2 * count // (CLU_DEV * groups)
    total = CLU_DEV * groups * most
    return pl.pallas_call(
        functools.partial(exchange_kernel, groups, most),
        out_shape=jax.ShapeDtypeStruct((count,), jnp.float32),
        in_specs=[
            pl.BlockSpec(memory_space=pl.ANY),
            pl.BlockSpec(memory_space=pltpu.VMEM),
        ],
        out_specs=pl.BlockSpec(memory_space=pltpu.VMEM),
        scratch_shapes=[
            pltpu.VMEM((count, width), jnp.bfloat16),
            pltpu.VMEM((total, width), jnp.bfloat16),
            pltpu.VMEM((total, width), jnp.bfloat16),
            pltpu.VMEM((1, 1, total), jnp.float32),
            pltpu.VMEM((groups, 1, LANES), jnp.float32),
            pltpu.SemaphoreType.DMA((4,)),
            pltpu.SemaphoreType.DMA((groups,)),
            pltpu.SemaphoreType.DMA((groups,)),
            pltpu.SemaphoreType.DMA((groups,)),
            pltpu.SemaphoreType.DMA((groups,)),
            pltpu.SemaphoreType.REGULAR((groups.bit_length(), groups.bit_length())),
        ],
        compiler_params=pltpu.CompilerParams(collective_id=0, has_side_effects=True),
    )(embeddings, assignment.reshape(1, count))


def slot_index(cluster, groups, most):
    count = cluster.shape[0]
    order = jnp.argsort(cluster, stable=True)
    ranked = cluster[order]
    first = jnp.searchsorted(ranked, ranked, side="left")
    rank_sorted = jnp.arange(count, dtype=jnp.int32) - first
    rank = jnp.zeros((count,), jnp.int32).at[order].set(rank_sorted)
    local = cluster % CLU_DEV
    owner = cluster // CLU_DEV
    return (local * groups + owner) * most + rank


def cluster_scores(pieces):
    rows, flags = pieces
    items = rows.shape[0]
    width = rows.shape[1] * rows.shape[2]
    rows = rows.reshape(items, width, rows.shape[3])
    flags = flags.reshape(items, width)
    offsets = jnp.arange(width, dtype=jnp.int32)
    distinct = offsets[:, None] != offsets[None, :]

    def single(pair):
        block, marks = pair
        gram = lax.dot_general(
            block, block, (((1,), (1,)), ((), ())), preferred_element_type=jnp.float32
        )
        keep = distinct & (marks > 0)[None, :]
        best = jnp.max(jnp.where(keep, gram, jnp.float32(-2.0)), axis=1)
        return jnp.maximum(best, jnp.float32(-1.0))

    best = lax.map(single, (rows, flags))
    return best.reshape(items, 1, width)


def general_shards(embeddings, assignment):
    groups = lax.axis_size("clu")
    count = embeddings.shape[0]
    width = embeddings.shape[1]
    most = 2 * count // (CLU_DEV * groups)
    unit = normalize(embeddings)
    cluster = assignment[:, 0]
    slot = slot_index(cluster, groups, most)
    total = CLU_DEV * groups * most
    outgoing = jnp.zeros((total, width), jnp.bfloat16).at[slot].set(unit)
    marks = jnp.zeros((total,), jnp.bfloat16).at[slot].set(jnp.ones((count,), jnp.bfloat16))
    outgoing = outgoing.reshape(CLU_DEV, groups, most, width)
    marks = marks.reshape(CLU_DEV, groups, most)
    arrived = (
        lax.all_to_all(outgoing, "clu", split_axis=1, concat_axis=2, tiled=True),
        lax.all_to_all(marks, "clu", split_axis=1, concat_axis=2, tiled=True),
    )
    best = cluster_scores(arrived)
    returned = lax.all_to_all(best, "clu", split_axis=2, concat_axis=1, tiled=True)
    return returned.reshape(total)[slot]


def shards(embeddings, assignment):
    groups = lax.axis_size("clu")
    count = embeddings.shape[0]
    most = 2 * count // (CLU_DEV * groups)
    block = CLU_DEV * most
    power = groups & (groups - 1) == 0 and most & (most - 1) == 0
    if power and block % 16 == 0 and LANES % block == 0 and (groups * block) % LANES == 0:
        return kernel_shards(embeddings, assignment)
    return general_shards(embeddings, assignment)


def solution(mesh):
    in_specs = (P(("lang", "clu"), None), P(("lang", "clu"), None))
    out_specs = P(("lang", "clu"))
    return jax.shard_map(shards, mesh=mesh, in_specs=in_specs, out_specs=out_specs, check_vma=False)
```
